128 devices in a mesh: att: 4 (over x), emb: 32 (over z, y, core).
Axes of the slice: x: 4, y: 4, z: 4, core: 2. Of those that a mesh axis runs over, the one named last changes fastest.
Arguments:
- w_qkv: float32 [4, 3, 2560, 2048], P(None, None, 'emb', 'att')
- w_out: float32 [4, 2048, 2560], P(None, 'att', 'emb')
- x_in: bfloat16 [4, 6144, 2560], P(None, None, 'emb')
- dy_qkv: bfloat16 [4, 3, 6144, 2048], P(None, None, None, 'att')
- x_attn: bfloat16 [4, 6144, 2048], P(None, None, 'att')
- dy_out: bfloat16 [4, 6144, 2560], P(None, None, 'emb')
- r_qkv: float32 [4, 3, 2560], P(None, None, 'emb')
- c_qkv: float32 [4, 3, 2048], P(None, None, 'att')
- r_out: float32 [4, 2048], P(None, 'att')
- c_out: float32 [4, 2560], P(None, 'emb')
- hyper_params: float32 [3], replicated
Outputs:
- output 1: float32 [4, 3, 2560, 2048], P(None, None, 'emb', 'att')
- output 2: float32 [4, 2048, 2560], P(None, 'att', 'emb')
- output 3: float32 [4, 3, 2560], P(None, None, 'emb')
- output 4: float32 [4, 3, 2048], P(None, None, 'att')
- output 5: float32 [4, 2048], P(None, 'att')
- output 6: float32 [4, 2560], P(None, 'emb')
All inputs are finite; a program needn't handle non-finite values.
Results may differ from the reference program's by a relative error of at most 0.001.
Values are sent between devices in bfloat16 or wider.
A program may use at most 1 GiB of HBM per device.

```python
import functools
import jax
import jax.numpy as jnp
from jax import lax

D = 2560
HEADS = 32
HEAD = 64
TOKENS = 6144
LAYERS = 4

INNER = HEADS * HEAD
EPS_SQUARE = 1e-30
EPS_SCALE = 1e-3


def cos_scale(rng_key, lead_shape, length, amplitude):
    phase_off = jax.random.uniform(rng_key, lead_shape + (1,), jnp.float32)
    position = jnp.arange(length, dtype=jnp.float32) / length
    return jnp.exp(amplitude * jnp.cos(2.0 * jnp.pi * (position + phase_off)))


def scaled_tokens(rng_key, lead_shape, length, factor):
    key_noise, key_scale = jax.random.split(rng_key)
    gauss_noise = jax.random.normal(key_noise, lead_shape + (2, TOKENS // 2, length), jnp.float32)
    scales = cos_scale(key_scale, lead_shape + (2, 1), length, 0.75)
    return (gauss_noise * scales * factor).reshape(lead_shape + (TOKENS, length)).astype(jnp.bfloat16)


def scaled_weight(rng_key, lead_shape, n_rows, n_cols):
    key_noise, key_row, key_col = jax.random.split(rng_key, 3)
    gauss_noise = jax.random.normal(key_noise, lead_shape + (n_rows, n_cols), jnp.float32)
    row_scale = cos_scale(key_row, lead_shape, n_rows, 0.5)
    col_scale = cos_scale(key_col, lead_shape, n_cols, 0.5)
    return gauss_noise * row_scale[..., :, None] * col_scale[..., None, :] * n_rows ** -0.5


def setup_inputs(seed: int = 0) -> dict:
    key_list = jax.random.split(jax.random.key(seed), 11)
    tok_norm = TOKENS ** -0.5
    low_end = jnp.array([0.5, 0.5, 0.2], jnp.float32)
    high_end = jnp.array([0.8, 1.0, 0.4], jnp.float32)
    return {
        "w_qkv": scaled_weight(key_list[0], (LAYERS, 3), D, INNER),
        "w_out": scaled_weight(key_list[1], (LAYERS,), INNER, D),
        "x_in": scaled_tokens(key_list[2], (LAYERS,), D, 1.0),
        "dy_qkv": scaled_tokens(key_list[3], (LAYERS, 3), INNER, tok_norm),
        "x_attn": scaled_tokens(key_list[4], (LAYERS,), INNER, 1.0),
        "dy_out": scaled_tokens(key_list[5], (LAYERS,), D, tok_norm),
        "r_qkv": jax.random.uniform(key_list[6], (LAYERS, 3, D), jnp.float32, 0.2, 1.0),
        "c_qkv": jax.random.uniform(key_list[7], (LAYERS, 3, INNER), jnp.float32, 0.2, 1.0),
        "r_out": jax.random.uniform(key_list[8], (LAYERS, INNER), jnp.float32, 0.2, 1.0),
        "c_out": jax.random.uniform(key_list[9], (LAYERS, D), jnp.float32, 0.2, 1.0),
        "hyper_params": jax.random.uniform(key_list[10], (3,), jnp.float32, low_end, high_end),
    }


def adafactor_one(w_grad, weight, row_old, col_old, hyper_params):
    beta_two = hyper_params[0]
    rel_step = hyper_params[1]
    clip_limit = hyper_params[2]
    q_sq = w_grad * w_grad + EPS_SQUARE
    row_new = beta_two * row_old + (1.0 - beta_two) * jnp.mean(q_sq, axis=1)
    col_new = beta_two * col_old + (1.0 - beta_two) * jnp.mean(q_sq, axis=0)
    second = row_new[:, None] * col_new[None, :] / jnp.mean(row_new)
    update = w_grad / jnp.sqrt(second)
    rms_u = jnp.sqrt(jnp.mean(update * update))
    clipped = update / jnp.maximum(1.0, rms_u / clip_limit)
    step_size = rel_step * jnp.maximum(EPS_SCALE, jnp.sqrt(jnp.mean(weight * weight)))
    return weight - step_size * clipped, row_new, col_new


def reference(w_qkv, w_out, x_in, dy_qkv, x_attn, dy_out, r_qkv, c_qkv, r_out, c_out, hyper_params):
    step_fn = functools.partial(adafactor_one, hyper_params=hyper_params)

    def one_layer(carry, layer_in):
        lw_qkv, lw_out, lx_in, ldy_qkv, lx_attn, ldy_out, lr_qkv, lc_qkv, lr_out, lc_out = layer_in
        g_qkv = jnp.einsum("td,ktn->kdn", lx_in.astype(jnp.float32), ldy_qkv.astype(jnp.float32))
        g_out = jnp.dot(lx_attn.T, ldy_out, preferred_element_type=jnp.float32)
        new_qkv = jax.vmap(step_fn)(g_qkv, lw_qkv, lr_qkv, lc_qkv)
        new_out = step_fn(g_out, lw_out, lr_out, lc_out)
        return carry, (new_qkv[0], new_out[0], new_qkv[1], new_qkv[2], new_out[1], new_out[2])

    final_carry, results = lax.scan(
        one_layer,
        jnp.zeros((), jnp.float32),
        (w_qkv, w_out, x_in, dy_qkv, x_attn, dy_out, r_qkv, c_qkv, r_out, c_out),
    )
    return (results[0], results[1], results[2], results[3], results[4], results[5])
```

```python
import functools
import jax
import jax.numpy as jnp
from jax import lax
from jax.experimental import pallas as pl
from jax.experimental.pallas import tpu as pltpu
from jax.sharding import PartitionSpec as P

EPS_SQUARE = 1e-30
EPS_SCALE = 1e-3
LANES = 128
MATS = 4
SLOTS = 3
PIECES = 4
MESH = pl.DeviceIdType.MESH


def adafactor_kernel(
    n_att, n_emb,
    xt, dt, dyq, xa, wq, wo, rq, cq, ro, co, hyp,
    wq_new, wo_new, rq_new, cq_new, ro_new, co_new,
    bbuf, abuf, g, wqv, wov, rqv, cqv, rov, cov, hv, qrecv, precv, urecv,
    bsem, asem, wsem, ssem, qsend_sem, qrecv_sem, psend_sem, precv_sem, usend_sem, urecv_sem,
):
    layers, p_loc, tokens = xt.shape
    q_loc = dyq.shape[3]
    n_mats = layers * MATS
    n_dev = n_att * n_emb
    d_model, inner = p_loc * n_emb, q_loc * n_att
    rows = tokens // PIECES
    q_rows = q_loc // LANES
    me_a, me_e = lax.axis_index("att"), lax.axis_index("emb")
    me = me_a * n_emb + me_e

    def device_of(flat):
        return {"att": flat // n_emb, "emb": lax.rem(flat, n_emb)}

    barrier = pltpu.get_barrier_semaphore()

    def greet(j, carry):
        pl.semaphore_signal(barrier, inc=1, device_id=device_of(lax.rem(me + j, n_dev)), device_id_type=MESH)
        return carry

    lax.fori_loop(1, n_dev, greet, 0)

    def start_a(src, layer, slot):
        pltpu.make_async_copy(src.at[layer], abuf.at[slot], asem.at[slot]).start()

    def start_b(mat, slot):
        layer, kind = mat // MATS, lax.rem(mat, MATS)

        def pieces(src):
            for k in range(PIECES):
                part = pl.ds(k * rows, rows)
                pltpu.make_async_copy(src.at[part], bbuf.at[slot, part], bsem.at[slot, k]).start()

        @pl.when(kind < MATS - 1)
        def _():
            pieces(dyq.at[layer, kind])

        @pl.when(kind == MATS - 1)
        def _():
            pieces(xa.at[layer])

    start_a(xt, 0, 0)
    for mat in range(SLOTS):
        for k in range(PIECES):
            part = pl.ds(k * rows, rows)
            pltpu.make_async_copy(dyq.at[0, mat, part], bbuf.at[mat, part], bsem.at[mat, k]).start()
    start_a(dt, 0, 1)
    small = [
        pltpu.make_async_copy(src, dst, ssem.at[k])
        for k, (src, dst) in enumerate([(rq, rqv), (cq, cqv), (ro, rov), (co, cov), (hyp, hv)])
    ]
    w_copies = [pltpu.make_async_copy(wq, wqv, wsem.at[0]), pltpu.make_async_copy(wo, wov, wsem.at[1])]
    for copy in small + w_copies:
        copy.start()

    def stream(mat, carry):
        slot = lax.rem(mat, SLOTS)
        layer, kind = mat // MATS, lax.rem(mat, MATS)
        a_slot = 2 * layer + kind // (MATS - 1)

        @pl.when(lax.rem(kind, MATS - 1) == 0)
        def _():
            pltpu.make_async_copy(xt.at[0], abuf.at[a_slot], asem.at[a_slot]).wait()

        @pl.when((kind == 0) & (layer < layers - 1))
        def _():
            start_a(xt, layer + 1, 2 * layer + 2)
            start_a(dt, layer + 1, 2 * layer + 3)

        acc = jnp.zeros((p_loc, q_loc), jnp.float32)
        for k in range(PIECES):
            part = pl.ds(k * rows, rows)
            pltpu.make_async_copy(dyq.at[0, 0, part], bbuf.at[slot, part], bsem.at[slot, k]).wait()
            acc += jnp.dot(abuf[a_slot, :, part], bbuf[slot, part, :], preferred_element_type=jnp.float32)
        g[mat] = acc

        @pl.when(mat + SLOTS < n_mats)
        def _():
            start_b(mat + SLOTS, slot)

        q_sq = acc * acc + EPS_SQUARE
        q_part = jnp.sum(q_sq, axis=0, keepdims=True)
        folded = q_sq[:, :LANES]
        for k in range(1, q_rows):
            folded += q_sq[:, k * LANES:(k + 1) * LANES]
        padded = jnp.concatenate([folded, jnp.zeros((LANES - p_loc, LANES), jnp.float32)], axis=0)
        for k in range(q_rows):
            qrecv[me_e, mat, k:k + 1, :] = q_part[:, k * LANES:(k + 1) * LANES]
        precv[me_a, mat] = jnp.sum(padded.T, axis=0, keepdims=True)
        return carry

    def q_copy(lo, hi, event, peer):
        span = qrecv.at[me_e, pl.ds(lo, hi - lo)]
        return pltpu.make_async_remote_copy(
            src_ref=span, dst_ref=span, send_sem=qsend_sem.at[event], recv_sem=qrecv_sem.at[event],
            device_id={"att": me_a, "emb": peer}, device_id_type=MESH)

    def p_copy(lo, hi, event, peer):
        span = precv.at[me_a, pl.ds(lo, hi - lo)]
        return pltpu.make_async_remote_copy(
            src_ref=span, dst_ref=span, send_sem=psend_sem.at[event], recv_sem=precv_sem.at[event],
            device_id={"att": peer, "emb": me_e}, device_id_type=MESH)

    def u_copy(flat):
        return pltpu.make_async_remote_copy(
            src_ref=urecv.at[me], dst_ref=urecv.at[me], send_sem=usend_sem, recv_sem=urecv_sem,
            device_id=device_of(flat), device_id_type=MESH)

    def send(lo, hi, event):
        def to_emb(j, carry):
            q_copy(lo, hi, event, lax.rem(me_e + j, n_emb)).start()
            return carry

        def to_att(j, carry):
            p_copy(lo, hi, event, lax.rem(me_a + j, n_att)).start()
            return carry

        lax.fori_loop(1, n_emb, to_emb, 0)
        lax.fori_loop(1, n_att, to_att, 0)

    def wait_bytes(ref, sem):
        pltpu.make_async_copy(ref, ref, sem).wait()

    lane = lax.broadcasted_iota(jnp.int32, (1, LANES), 1)

    def process(lo, hi, event, u_row):
        wait_bytes(qrecv.at[pl.ds(0, n_emb - 1), pl.ds(lo, hi - lo)], qrecv_sem.at[event])
        wait_bytes(precv.at[pl.ds(0, n_att - 1), pl.ds(lo, hi - lo)], precv_sem.at[event])
        beta = hv[0:1, 0:1]
        for mat in range(lo, hi):
            layer, kind = mat // MATS, mat % MATS
            is_out = kind == MATS - 1
            q_sum = qrecv[0, mat]
            for peer in range(1, n_emb):
                q_sum += qrecv[peer, mat]
            p_sum = precv[0, mat]
            for peer in range(1, n_att):
                p_sum += precv[peer, mat]
            q_add = (1.0 - beta) * (q_sum / d_model)
            p_new_all = (1.0 - beta) * (p_sum / inner)
            p_old = cov[layer:layer + 1, :] if is_out else rqv[kind, layer:layer + 1, :]
            p_new = beta * p_old + p_new_all[:, :p_loc]
            q_parts = []
            for k in range(q_rows):
                cols = slice(k * LANES, (k + 1) * LANES)
                q_old = rov[layer:layer + 1, cols] if is_out else cqv[kind, layer:layer + 1, cols]
                q_new = beta * q_old + q_add[k:k + 1, :]
                if is_out:
                    ro_new[layer:layer + 1, cols] = q_new
                else:
                    cq_new[kind, layer:layer + 1, cols] = q_new
                q_parts.append(q_new)
            if is_out:
                co_new[layer:layer + 1, :] = p_new
                r_total = jnp.sum(sum(q_parts[1:], q_parts[0]), axis=1, keepdims=True)
            else:
                rq_new[kind, layer:layer + 1, :] = p_new
                r_total = jnp.sum(p_new, axis=1, keepdims=True)
            p_fac = jnp.concatenate([lax.rsqrt(p_new), jnp.zeros((1, LANES - p_loc), jnp.float32)], axis=1)
            p_fac = jnp.broadcast_to(p_fac, (LANES, LANES)).T[:p_loc, :]
            u_sum = jnp.zeros((p_loc, LANES), jnp.float32)
            w_sum = jnp.zeros((p_loc, LANES), jnp.float32)
            for k in range(q_rows):
                cols = slice(k * LANES, (k + 1) * LANES)
                upd = (g[mat, :, cols] * p_fac) * lax.rsqrt(q_parts[k])
                g[mat, :, cols] = upd
                w = wov[layer, :, cols] if is_out else wqv[layer, kind, :, cols]
                u_sum += upd * upd
                w_sum += w * w
            u_total = jnp.sum(jnp.sum(u_sum, axis=0, keepdims=True), axis=1, keepdims=True)
            w_total = jnp.sum(jnp.sum(w_sum, axis=0, keepdims=True), axis=1, keepdims=True)
            copies = n_emb if is_out else n_att
            mean_row = r_total / (copies * (inner if is_out else d_model))
            u_row = jnp.where(lane == mat, u_total, u_row)
            u_row = jnp.where(lane == n_mats + mat, w_total, u_row)
            u_row = jnp.where(lane == 2 * n_mats + mat, mean_row, u_row)
        return u_row

    groups = [(MATS * layer, MATS * (layer + 1)) for layer in range(layers - 1)]
    groups += [(n_mats - MATS, n_mats - 1), (n_mats - 1, n_mats)]
    u_row = jnp.zeros((1, LANES), jnp.float32)
    for event, (lo, hi) in enumerate(groups):
        lax.fori_loop(lo, hi, stream, 0)
        if event == 0:
            pl.semaphore_wait(barrier, n_dev - 1)
        send(lo, hi, event)
        if event == 0:
            for copy in small + w_copies:
                copy.wait()
        else:
            u_row = process(*groups[event - 1], event - 1, u_row)
    u_row = process(*groups[-1], len(groups) - 1, u_row)

    urecv[me] = u_row

    def to_all(j, carry):
        u_copy(lax.rem(me + j, n_dev)).start()
        return carry

    lax.fori_loop(1, n_dev, to_all, 0)
    wait_bytes(urecv.at[pl.ds(0, n_dev - 1)], urecv_sem)
    total = urecv[0]
    for peer in range(1, n_dev):
        total += urecv[peer]
    w_total = pltpu.roll(total, LANES - n_mats, 1)
    mean_row = pltpu.roll(total, LANES - 2 * n_mats, 1)
    n_elems = d_model * inner
    rel_step, clip_limit = hv[0:1, 1:2], hv[0:1, 2:3]
    rms_u = jnp.sqrt(mean_row * total / n_elems)
    rms_w = jnp.sqrt(w_total / n_elems)
    scale = rel_step * jnp.maximum(EPS_SCALE, rms_w) / jnp.maximum(1.0, rms_u / clip_limit) * jnp.sqrt(mean_row)
    for mat in range(n_mats):
        layer, kind = mat // MATS, mat % MATS
        factor = scale[:, mat:mat + 1]
        if kind == MATS - 1:
            wo_new[layer] = wov[layer] - factor * g[mat]
        else:
            wq_new[layer, kind] = wqv[layer, kind] - factor * g[mat]

    for event, (lo, hi) in enumerate(groups):
        wait_bytes(qrecv.at[pl.ds(0, n_emb - 1), pl.ds(lo, hi - lo)], qsend_sem.at[event])
        wait_bytes(precv.at[pl.ds(0, n_att - 1), pl.ds(lo, hi - lo)], psend_sem.at[event])
    wait_bytes(urecv.at[pl.ds(0, n_dev - 1)], usend_sem)


def solution(mesh):
    n_emb = mesh.shape["emb"]
    n_att = mesh.shape["att"]
    in_specs = (
        P(None, None, "emb", "att"),
        P(None, "att", "emb"),
        P(None, None, "emb"),
        P(None, None, None, "att"),
        P(None, None, "att"),
        P(None, None, "emb"),
        P(None, None, "emb"),
        P(None, None, "att"),
        P(None, "att"),
        P(None, "emb"),
        P(),
    )
    out_specs = (
        P(None, None, "emb", "att"),
        P(None, "att", "emb"),
        P(None, None, "emb"),
        P(None, None, "att"),
        P(None, "att"),
        P(None, "emb"),
    )

    def local_run(w_qkv, w_out, x_in, dy_qkv, x_attn, dy_out, r_qkv, c_qkv, r_out, c_out, hyper_params):
        f32, bf16 = jnp.float32, jnp.bfloat16
        layers, tokens, p_loc = x_in.shape
        q_loc = x_attn.shape[2]
        n_mats, n_groups = layers * MATS, layers + 1
        args = (
            jnp.swapaxes(x_in, 1, 2), jnp.swapaxes(dy_out, 1, 2), dy_qkv, x_attn,
            w_qkv, jnp.swapaxes(w_out, 1, 2),
            jnp.swapaxes(r_qkv, 0, 1), jnp.swapaxes(c_qkv, 0, 1), r_out, c_out, hyper_params.reshape(1, 3),
        )
        sds = jax.ShapeDtypeStruct
        wo_shape = (layers, p_loc, q_loc)
        rq_shape, cq_shape = (3, layers, p_loc), (3, layers, q_loc)
        out_shape = (
            sds(w_qkv.shape, f32), sds(wo_shape, f32), sds(rq_shape, f32), sds(cq_shape, f32),
            sds(r_out.shape, f32), sds(c_out.shape, f32),
        )
        dma = pltpu.SemaphoreType.DMA
        outs = pl.pallas_call(
            functools.partial(adafactor_kernel, n_att, n_emb),
            out_shape=out_shape,
            in_specs=[pl.BlockSpec(memory_space=pltpu.HBM)] * len(args),
            out_specs=[pl.BlockSpec(memory_space=pltpu.VMEM)] * len(out_shape),
            scratch_shapes=[
                pltpu.VMEM((SLOTS, tokens, q_loc), bf16),
                pltpu.VMEM((2 * layers, p_loc, tokens), bf16),
                pltpu.VMEM((n_mats, p_loc, q_loc), f32),
                pltpu.VMEM(w_qkv.shape, f32),
                pltpu.VMEM(wo_shape, f32),
                pltpu.VMEM(rq_shape, f32),
                pltpu.VMEM(cq_shape, f32),
                pltpu.VMEM(r_out.shape, f32),
                pltpu.VMEM(c_out.shape, f32),
                pltpu.VMEM((1, 3), f32),
                pltpu.VMEM((n_emb, n_mats, q_loc // LANES, LANES), f32),
                pltpu.VMEM((n_att, n_mats, 1, LANES), f32),
                pltpu.VMEM((n_att * n_emb, 1, LANES), f32),
                dma((SLOTS, PIECES)), dma((2 * layers,)), dma((2,)), dma((5,)),
                dma((n_groups,)), dma((n_groups,)), dma((n_groups,)), dma((n_groups,)), dma(()), dma(()),
            ],
            compiler_params=pltpu.CompilerParams(
                collective_id=0, has_side_effects=True, vmem_limit_bytes=48 * 1024 * 1024),
            name="adafactor",
        )(*args)
        return (
            outs[0], jnp.swapaxes(outs[1], 1, 2), jnp.swapaxes(outs[2], 0, 1), jnp.swapaxes(outs[3], 0, 1),
            outs[4], outs[5],
        )

    return jax.shard_map(local_run, mesh=mesh, in_specs=in_specs, out_specs=out_specs, check_vma=False)
```

```python
import functools
import jax
import jax.numpy as jnp
from jax import lax
from jax.experimental import pallas as pl
from jax.experimental.pallas import tpu as pltpu
from jax.sharding import PartitionSpec as P

EPS_SQUARE = 1e-30
EPS_SCALE = 1e-3
LANES = 128
MATS = 4
SLOTS = 4
PIECES = 6
RING = 6
LEAD = 3
MESH = pl.DeviceIdType.MESH


def adafactor_kernel(
    n_att, n_emb,
    xt, dt, dyq, xa, wq, wo, rq, cq, ro, co, hyp,
    wqv, wov, g, scale_row, rq_new, cq_new, ro_new, co_new,
    bbuf, fbuf, rbuf, abuf, rqv, cqv, rov, cov, hv, qrecv, precv, urecv,
    bsem, fsem, fsend_sem, rsem, free_sem, asem, wsem, ssem,
    qsend_sem, qrecv_sem, psend_sem, precv_sem, usend_sem, urecv_sem,
):
    layers, p_loc, tokens = xt.shape
    q_loc = dyq.shape[3]
    n_mats = layers * MATS
    n_dev = n_att * n_emb
    d_model, inner = p_loc * n_emb, q_loc * n_att
    rows, main = tokens // PIECES, PIECES - 2
    q_rows = q_loc // LANES
    me_a, me_e = lax.axis_index("att"), lax.axis_index("emb")
    me = me_a * n_emb + me_e
    core = lax.rem(me_e, 2)
    partner = {"att": me_a, "emb": me_e + 1 - 2 * core}
    own_part = pl.ds(pl.multiple_of((PIECES - 1 - core) * rows, rows), rows)
    got_part = pl.ds(pl.multiple_of((PIECES - 2 + core) * rows, rows), rows)

    def start_a(src, layer, slot):
        pltpu.make_async_copy(src.at[layer], abuf.at[slot], asem.at[slot]).start()

    def start_pass(src, slot):
        pltpu.make_async_copy(src.at[own_part], fbuf.at[slot], fsem.at[slot]).start()

    def start_main(src, slot):
        for k in range(main):
            part = pl.ds(k * rows, rows)
            pltpu.make_async_copy(src.at[part], bbuf.at[slot, part], bsem.at[slot, k]).start()

    def of_mat(start, mat, slot):
        layer, kind = mat // MATS, lax.rem(mat, MATS)

        @pl.when(kind < MATS - 1)
        def _():
            start(dyq.at[layer, kind], slot)

        @pl.when(kind == MATS - 1)
        def _():
            start(xa.at[layer], slot)

    def source(mat):
        return xa.at[mat // MATS] if mat % MATS == MATS - 1 else dyq.at[mat // MATS, mat % MATS]

    start_a(xt, 0, 0)
    for mat in range(SLOTS):
        start_pass(source(mat), mat)
        start_main(source(mat), mat)
    start_a(dt, 0, 1)
    for mat in range(SLOTS, RING):
        start_pass(source(mat), mat)
    small = [
        pltpu.make_async_copy(src, dst, ssem.at[k])
        for k, (src, dst) in enumerate([(rq, rqv), (cq, cqv), (ro, rov), (co, cov), (hyp, hv)])
    ]
    w_copies = [pltpu.make_async_copy(wq, wqv, wsem.at[0]), pltpu.make_async_copy(wo, wov, wsem.at[1])]
    for copy in small + w_copies:
        copy.start()

    side = 4
    att_at = [lax.rem(me_a + k, n_att) for k in range(n_att)]
    planes = n_emb // (2 * side)
    z_at = [lax.rem(me_e // (2 * side) + k, planes) * (2 * side) for k in range(planes)]
    y_at = [lax.rem(lax.rem(me_e, 2 * side) // 2 + k, side) * 2 for k in range(side)]
    core_at = [core, 1 - core]

    def hops(k, n):
        return min(k, n - k)

    emb_steps = sorted(
        ((z, y, h) for z in range(planes) for y in range(side) for h in range(2) if (z, y, h) != (0, 0, 0)),
        key=lambda s: -(hops(s[0], planes) + hops(s[1], side)))
    emb_at = {(z, y, h): z_at[z] + y_at[y] + core_at[h] for z in range(planes) for y in range(side) for h in range(2)}
    all_steps = sorted(
        ((k, s) for k in range(n_att) for s in emb_at if (k, s) != (0, (0, 0, 0))),
        key=lambda t: -(hops(t[0], n_att) + hops(t[1][0], planes) + hops(t[1][1], side)))

    barrier = pltpu.get_barrier_semaphore()
    for k, s in all_steps:
        pl.semaphore_signal(
            barrier, inc=1, device_id={"att": att_at[k], "emb": emb_at[s]}, device_id_type=MESH)
    pl.semaphore_wait(barrier, n_dev - 1)

    def pass_copy(slot):
        return pltpu.make_async_remote_copy(
            src_ref=fbuf.at[slot], dst_ref=rbuf.at[slot], send_sem=fsend_sem.at[slot], recv_sem=rsem.at[slot],
            device_id=partner, device_id_type=MESH)

    def pass_on(slot):
        pltpu.make_async_copy(dyq.at[0, 0, pl.ds(0, rows)], fbuf.at[slot], fsem.at[slot]).wait()
        pass_copy(slot).start()

    for mat in range(LEAD):
        pass_on(mat)

    def stream(mat, carry):
        slot, ring = lax.rem(mat, SLOTS), lax.rem(mat, RING)
        layer, kind = mat // MATS, lax.rem(mat, MATS)
        a_slot = 2 * layer + kind // (MATS - 1)
        ahead = mat + LEAD

        @pl.when(ahead < n_mats)
        def _():
            @pl.when(ahead >= RING)
            def _():
                pl.semaphore_wait(free_sem, 1)

            pass_on(lax.rem(ahead, RING))

        @pl.when(lax.rem(kind, MATS - 1) == 0)
        def _():
            pltpu.make_async_copy(xt.at[0], abuf.at[a_slot], asem.at[a_slot]).wait()

        @pl.when((kind == 0) & (layer < layers - 1))
        def _():
            start_a(xt, layer + 1, 2 * layer + 2)
            start_a(dt, layer + 1, 2 * layer + 3)

        def product(a_part, b):
            return jnp.dot(abuf[a_slot, :, a_part], b, preferred_element_type=jnp.float32)

        acc = product(own_part, fbuf[ring])
        for k in range(main):
            part = pl.ds(k * rows, rows)
            pltpu.make_async_copy(dyq.at[0, 0, part], bbuf.at[slot, part], bsem.at[slot, k]).wait()
            acc += product(part, bbuf[slot, part, :])
        pass_copy(ring).wait_recv()
        acc += product(got_part, rbuf[ring])
        g[mat] = acc

        @pl.when(mat + RING < n_mats)
        def _():
            pl.semaphore_signal(free_sem, inc=1, device_id=partner, device_id_type=MESH)
            pass_copy(ring).wait_send()
            of_mat(start_pass, mat + RING, ring)

        @pl.when(mat + SLOTS < n_mats)
        def _():
            of_mat(start_main, mat + SLOTS, slot)

        q_sq = acc * acc + EPS_SQUARE
        q_part = jnp.sum(q_sq, axis=0, keepdims=True)
        folded = q_sq[:, :LANES]
        for k in range(1, q_rows):
            folded += q_sq[:, k * LANES:(k + 1) * LANES]
        padded = jnp.concatenate([folded, jnp.zeros((LANES - p_loc, LANES), jnp.float32)], axis=0)
        for k in range(q_rows):
            qrecv[me_e, mat, k:k + 1, :] = q_part[:, k * LANES:(k + 1) * LANES]
        precv[me_a, mat] = jnp.sum(padded.T, axis=0, keepdims=True)
        return carry

    def q_copy(lo, hi, event, peer):
        span = qrecv.at[me_e, pl.ds(lo, hi - lo)]
        return pltpu.make_async_remote_copy(
            src_ref=span, dst_ref=span, send_sem=qsend_sem.at[event], recv_sem=qrecv_sem.at[event],
            device_id={"att": me_a, "emb": peer}, device_id_type=MESH)

    def p_copy(lo, hi, event, peer):
        span = precv.at[me_a, pl.ds(lo, hi - lo)]
        return pltpu.make_async_remote_copy(
            src_ref=span, dst_ref=span, send_sem=psend_sem.at[event], recv_sem=precv_sem.at[event],
            device_id={"att": peer, "emb": me_e}, device_id_type=MESH)

    def u_copy(target):
        return pltpu.make_async_remote_copy(
            src_ref=urecv.at[me], dst_ref=urecv.at[me], send_sem=usend_sem, recv_sem=urecv_sem,
            device_id=target, device_id_type=MESH)

    def send(lo, hi, event):
        def to_emb(j, carry):
            q_copy(lo, hi, event, lax.rem(me_e + j, n_emb)).start()
            return carry

        if hi < n_mats:
            lax.fori_loop(1, n_emb, to_emb, 0)
        else:
            for s in emb_steps:
                q_copy(lo, hi, event, emb_at[s]).start()
        for k in range(1, n_att):
            p_copy(lo, hi, event, att_at[k]).start()

    def wait_bytes(ref, sem):
        pltpu.make_async_copy(ref, ref, sem).wait()

    lane = lax.broadcasted_iota(jnp.int32, (1, LANES), 1)

    def process(lo, hi, event, u_row):
        wait_bytes(qrecv.at[pl.ds(0, n_emb - 1), pl.ds(lo, hi - lo)], qrecv_sem.at[event])
        wait_bytes(precv.at[pl.ds(0, n_att - 1), pl.ds(lo, hi - lo)], precv_sem.at[event])
        beta = hv[0:1, 0:1]
        for mat in range(lo, hi):
            layer, kind = mat // MATS, mat % MATS
            is_out = kind == MATS - 1
            q_sum = qrecv[0, mat]
            for peer in range(1, n_emb):
                q_sum += qrecv[peer, mat]
            p_sum = precv[0, mat]
            for peer in range(1, n_att):
                p_sum += precv[peer, mat]
            q_add = (1.0 - beta) * (q_sum / d_model)
            p_new_all = (1.0 - beta) * (p_sum / inner)
            p_old = cov[layer:layer + 1, :] if is_out else rqv[kind, layer:layer + 1, :]
            p_new = beta * p_old + p_new_all[:, :p_loc]
            q_parts = []
            for k in range(q_rows):
                cols = slice(k * LANES, (k + 1) * LANES)
                q_old = rov[layer:layer + 1, cols] if is_out else cqv[kind, layer:layer + 1, cols]
                q_new = beta * q_old + q_add[k:k + 1, :]
                if is_out:
                    ro_new[layer:layer + 1, cols] = q_new
                else:
                    cq_new[kind, layer:layer + 1, cols] = q_new
                q_parts.append(q_new)
            if is_out:
                co_new[layer:layer + 1, :] = p_new
                r_total = jnp.sum(sum(q_parts[1:], q_parts[0]), axis=1, keepdims=True)
            else:
                rq_new[kind, layer:layer + 1, :] = p_new
                r_total = jnp.sum(p_new, axis=1, keepdims=True)
            p_fac = jnp.concatenate([lax.rsqrt(p_new), jnp.zeros((1, LANES - p_loc), jnp.float32)], axis=1)
            p_fac = jnp.broadcast_to(p_fac, (LANES, LANES)).T[:p_loc, :]
            u_sum = jnp.zeros((p_loc, LANES), jnp.float32)
            w_sum = jnp.zeros((p_loc, LANES), jnp.float32)
            for k in range(q_rows):
                cols = slice(k * LANES, (k + 1) * LANES)
                upd = (g[mat, :, cols] * p_fac) * lax.rsqrt(q_parts[k])
                g[mat, :, cols] = upd
                w = wov[layer, :, cols] if is_out else wqv[layer, kind, :, cols]
                u_sum += upd * upd
                w_sum += w * w
            u_total = jnp.sum(jnp.sum(u_sum, axis=0, keepdims=True), axis=1, keepdims=True)
            w_total = jnp.sum(jnp.sum(w_sum, axis=0, keepdims=True), axis=1, keepdims=True)
            copies = n_emb if is_out else n_att
            mean_row = r_total / (copies * (inner if is_out else d_model))
            u_row = jnp.where(lane == mat, u_total, u_row)
            u_row = jnp.where(lane == n_mats + mat, w_total, u_row)
            u_row = jnp.where(lane == 2 * n_mats + mat, mean_row, u_row)
        return u_row

    groups = [(MATS * layer, MATS * (layer + 1)) for layer in range(layers - 1)]
    groups += [(n_mats - MATS, n_mats - 2), (n_mats - 2, n_mats - 1), (n_mats - 1, n_mats)]
    u_row = jnp.zeros((1, LANES), jnp.float32)
    for event, (lo, hi) in enumerate(groups):
        lax.fori_loop(lo, hi, stream, 0)
        send(lo, hi, event)
    for copy in small + w_copies:
        copy.wait()
    for event, (lo, hi) in enumerate(groups):
        u_row = process(lo, hi, event, u_row)

    urecv[me] = u_row

    for k, s in all_steps:
        u_copy({"att": att_at[k], "emb": emb_at[s]}).start()
    wait_bytes(urecv.at[pl.ds(0, n_dev - 1)], urecv_sem)
    total = urecv[0]
    for peer in range(1, n_dev):
        total += urecv[peer]
    w_total = pltpu.roll(total, LANES - n_mats, 1)
    mean_row = pltpu.roll(total, LANES - 2 * n_mats, 1)
    n_elems = d_model * inner
    rel_step, clip_limit = hv[0:1, 1:2], hv[0:1, 2:3]
    rms_u = jnp.sqrt(mean_row * total / n_elems)
    rms_w = jnp.sqrt(w_total / n_elems)
    scale = rel_step * jnp.maximum(EPS_SCALE, rms_w) / jnp.maximum(1.0, rms_u / clip_limit) * jnp.sqrt(mean_row)
    scale_row[...] = scale

    for mat in range(n_mats - RING, n_mats):
        pass_copy(mat % RING).wait_send()
    for event, (lo, hi) in enumerate(groups):
        wait_bytes(qrecv.at[pl.ds(0, n_emb - 1), pl.ds(lo, hi - lo)], qsend_sem.at[event])
        wait_bytes(precv.at[pl.ds(0, n_att - 1), pl.ds(lo, hi - lo)], psend_sem.at[event])
    wait_bytes(urecv.at[pl.ds(0, n_dev - 1)], usend_sem)


def update_kernel(wqv, wov, g, scale_row, *refs):
    stats, wq_new, wo_new, stats_new, wq_out, wo_out, sems = refs[:4], refs[4], refs[5], refs[6:10], *refs[10:]
    copies = [pltpu.make_async_copy(src, dst, sems.at[k]) for k, (src, dst) in enumerate(zip(stats, stats_new))]
    for copy in copies:
        copy.start()
    for mat in range(g.shape[0]):
        layer, kind = mat // MATS, mat % MATS
        step = scale_row[:, mat:mat + 1] * g[mat]
        if kind == MATS - 1:
            wo_out[layer] = wov[layer] - step
            copy = pltpu.make_async_copy(wo_out.at[layer], wo_new.at[layer], sems.at[len(stats) + mat])
        else:
            wq_out[layer, kind] = wqv[layer, kind] - step
            copy = pltpu.make_async_copy(wq_out.at[layer, kind], wq_new.at[layer, kind], sems.at[len(stats) + mat])
        copy.start()
        copies.append(copy)
    for copy in copies:
        copy.wait()


def solution(mesh):
    n_emb = mesh.shape["emb"]
    n_att = mesh.shape["att"]
    in_specs = (
        P(None, None, "emb", "att"),
        P(None, "att", "emb"),
        P(None, None, "emb"),
        P(None, None, None, "att"),
        P(None, None, "att"),
        P(None, None, "emb"),
        P(None, None, "emb"),
        P(None, None, "att"),
        P(None, "att"),
        P(None, "emb"),
        P(),
    )
    out_specs = (
        P(None, None, "emb", "att"),
        P(None, "att", "emb"),
        P(None, None, "emb"),
        P(None, None, "att"),
        P(None, "att"),
        P(None, "emb"),
    )

    def local_run(w_qkv, w_out, x_in, dy_qkv, x_attn, dy_out, r_qkv, c_qkv, r_out, c_out, hyper_params):
        f32, bf16 = jnp.float32, jnp.bfloat16
        layers, tokens, p_loc = x_in.shape
        q_loc = x_attn.shape[2]
        n_mats, n_groups = layers * MATS, layers + 2
        rows = tokens // PIECES
        args = (
            jnp.swapaxes(x_in, 1, 2), jnp.swapaxes(dy_out, 1, 2), dy_qkv, x_attn,
            w_qkv, jnp.swapaxes(w_out, 1, 2),
            jnp.swapaxes(r_qkv, 0, 1), jnp.swapaxes(c_qkv, 0, 1), r_out, c_out, hyper_params.reshape(1, 3),
        )
        args = tuple(pltpu.with_memory_space_constraint(a, pltpu.HBM) for a in args)
        sds = jax.ShapeDtypeStruct
        wo_shape = (layers, p_loc, q_loc)
        rq_shape, cq_shape = (3, layers, p_loc), (3, layers, q_loc)
        w_shape = (sds(w_qkv.shape, f32), sds(wo_shape, f32))
        stat_shape = (sds(rq_shape, f32), sds(cq_shape, f32), sds(r_out.shape, f32), sds(c_out.shape, f32))
        held = (*w_shape, sds((n_mats, p_loc, q_loc), f32), sds((1, LANES), f32), *stat_shape)
        dma = pltpu.SemaphoreType.DMA
        outs = pl.pallas_call(
            functools.partial(adafactor_kernel, n_att, n_emb),
            out_shape=held,
            in_specs=[pl.BlockSpec(memory_space=pltpu.HBM)] * len(args),
            out_specs=[pl.BlockSpec(memory_space=pltpu.VMEM)] * len(held),
            scratch_shapes=[
                pltpu.VMEM((SLOTS, tokens - 2 * rows, q_loc), bf16),
                pltpu.VMEM((RING, rows, q_loc), bf16),
                pltpu.VMEM((RING, rows, q_loc), bf16),
                pltpu.VMEM((2 * layers, p_loc, tokens), bf16),
                pltpu.VMEM(rq_shape, f32),
                pltpu.VMEM(cq_shape, f32),
                pltpu.VMEM(r_out.shape, f32),
                pltpu.VMEM(c_out.shape, f32),
                pltpu.VMEM((1, 3), f32),
                pltpu.VMEM((n_emb, n_mats, q_loc // LANES, LANES), f32),
                pltpu.VMEM((n_att, n_mats, 1, LANES), f32),
                pltpu.VMEM((n_att * n_emb, 1, LANES), f32),
                dma((SLOTS, PIECES - 2)), dma((RING,)), dma((RING,)), dma((RING,)), pltpu.SemaphoreType.REGULAR,
                dma((2 * layers,)), dma((2,)), dma((5,)),
                dma((n_groups,)), dma((n_groups,)), dma((n_groups,)), dma((n_groups,)), dma(()), dma(()),
            ],
            compiler_params=pltpu.CompilerParams(
                collective_id=0, has_side_effects=True, vmem_limit_bytes=42 * 1024 * 1024),
            name="adafactor",
        )(*args)
        outs = pl.pallas_call(
            update_kernel,
            out_shape=(*w_shape, *stat_shape),
            in_specs=[pl.BlockSpec(memory_space=pltpu.VMEM)] * len(held),
            out_specs=[pl.BlockSpec(memory_space=pltpu.HBM)] * (len(w_shape) + len(stat_shape)),
            scratch_shapes=[
                pltpu.VMEM(w_qkv.shape, f32), pltpu.VMEM(wo_shape, f32), dma((len(stat_shape) + n_mats,)),
            ],
            compiler_params=pltpu.CompilerParams(vmem_limit_bytes=4 * 1024 * 1024),
            name="update",
        )(*outs)
        return (
            outs[0], jnp.swapaxes(outs[1], 1, 2), jnp.swapaxes(outs[2], 0, 1), jnp.swapaxes(outs[3], 0, 1),
            outs[4], outs[5],
        )

    return jax.shard_map(local_run, mesh=mesh, in_specs=in_specs, out_specs=out_specs, check_vma=False)
```

```python
import functools
import jax
import jax.numpy as jnp
from jax import lax
from jax.experimental import pallas as pl
from jax.experimental.pallas import tpu as pltpu
from jax.sharding import PartitionSpec as P

EPS_SQUARE = 1e-30
EPS_SCALE = 1e-3
LANES = 128
MATS = 4
SLOTS = 3
PIECES = 6
RING = 5
LEAD = 1
EARLY = 2
MESH = pl.DeviceIdType.MESH


def adafactor_kernel(
    n_att, n_emb,
    xt, dt, dyq, xa, wq, wo, rq, cq, ro, co, hyp,
    wqv, wov, g, scale_rows, rq_new, cq_new, ro_new, co_new,
    bbuf, fbuf, rbuf, abuf, rqv, cqv, rov, cov, hv, qrecv, precv, urecv,
    bsem, fsem, fsend_sem, rsem, free_sem, asem, wsem, ssem,
    qsend_sem, qrecv_sem, psend_sem, precv_sem, usend_sem, urecv_sem,
):
    layers, p_loc, tokens = xt.shape
    q_loc = dyq.shape[3]
    n_mats = layers * MATS
    n_dev = n_att * n_emb
    d_model, inner = p_loc * n_emb, q_loc * n_att
    rows, main = tokens // PIECES, PIECES - 2
    q_rows = q_loc // LANES
    me_a, me_e = lax.axis_index("att"), lax.axis_index("emb")
    me = me_a * n_emb + me_e
    core = lax.rem(me_e, 2)
    partner = {"att": me_a, "emb": me_e + 1 - 2 * core}
    own_part = pl.ds(pl.multiple_of((PIECES - 1 - core) * rows, rows), rows)
    got_part = pl.ds(pl.multiple_of((PIECES - 2 + core) * rows, rows), rows)

    def start_a(src, layer, slot):
        pltpu.make_async_copy(src.at[layer], abuf.at[slot], asem.at[slot]).start()

    def start_pass(src, slot):
        pltpu.make_async_copy(src.at[own_part], fbuf.at[slot], fsem.at[slot]).start()

    def start_got(src, slot):
        pltpu.make_async_copy(src.at[got_part], rbuf.at[slot], rsem.at[slot]).start()

    def start_piece(src, slot, k):
        part = pl.ds(k * rows, rows)
        pltpu.make_async_copy(src.at[part], bbuf.at[slot, part], bsem.at[slot, k]).start()

    def of_mat(start, mat, slot, *more):
        layer, kind = mat // MATS, lax.rem(mat, MATS)

        @pl.when(kind < MATS - 1)
        def _():
            start(dyq.at[layer, kind], slot, *more)

        @pl.when(kind == MATS - 1)
        def _():
            start(xa.at[layer], slot, *more)

    def source(mat):
        return xa.at[mat // MATS] if mat % MATS == MATS - 1 else dyq.at[mat // MATS, mat % MATS]

    start_a(xt, 0, 0)
    for k in range(main):
        start_piece(source(0), 0, k)
    start_pass(source(0), 0)
    start_got(source(0), 0)
    small = [
        pltpu.make_async_copy(src, dst, ssem.at[k])
        for k, (src, dst) in enumerate([(rq, rqv), (cq, cqv), (ro, rov), (co, cov), (hyp, hv)])
    ]
    w_copies = [pltpu.make_async_copy(wq, wqv, wsem.at[0]), pltpu.make_async_copy(wo, wov, wsem.at[1])]

    side = 4
    att_at = [lax.rem(me_a + k, n_att) for k in range(n_att)]
    planes = n_emb // (2 * side)
    z_at = [lax.rem(me_e // (2 * side) + k, planes) * (2 * side) for k in range(planes)]
    y_at = [lax.rem(lax.rem(me_e, 2 * side) // 2 + k, side) * 2 for k in range(side)]
    core_at = [core, 1 - core]

    def hops(k, n):
        return min(k, n - k)

    emb_steps = sorted(
        ((z, y, h) for z in range(planes) for y in range(side) for h in range(2) if (z, y, h) != (0, 0, 0)),
        key=lambda s: -(hops(s[0], planes) + hops(s[1], side)))
    emb_at = {(z, y, h): z_at[z] + y_at[y] + core_at[h] for z in range(planes) for y in range(side) for h in range(2)}
    all_steps = sorted(
        ((k, s) for k in range(n_att) for s in emb_at if (k, s) != (0, (0, 0, 0))),
        key=lambda t: -(hops(t[0], n_att) + hops(t[1][0], planes) + hops(t[1][1], side)))

    barrier = pltpu.get_barrier_semaphore()
    for k, s in all_steps:
        pl.semaphore_signal(
            barrier, inc=1, device_id={"att": att_at[k], "emb": emb_at[s]}, device_id_type=MESH)
    for k in range(main):
        start_piece(source(1), 1, k)
    start_pass(source(1), 1)
    start_got(source(1), 1)
    start_pass(source(EARLY), EARLY)

    def pass_copy(slot):
        return pltpu.make_async_remote_copy(
            src_ref=fbuf.at[slot], dst_ref=rbuf.at[slot], send_sem=fsend_sem.at[slot], recv_sem=rsem.at[slot],
            device_id=partner, device_id_type=MESH)

    def wait_pass(slot):
        pltpu.make_async_copy(dyq.at[0, 0, pl.ds(0, rows)], fbuf.at[slot], fsem.at[slot]).wait()

    def a_slot(mat):
        return 2 * lax.rem(mat // MATS, 2) + lax.rem(mat, MATS) // (MATS - 1)

    def product(mat, part, b):
        return jnp.dot(abuf[a_slot(mat), :, part], b, preferred_element_type=jnp.float32)

    def ready_a(mat):
        kind, layer = lax.rem(mat, MATS), mat // MATS

        @pl.when(lax.rem(kind, MATS - 1) == 0)
        def _():
            pltpu.make_async_copy(xt.at[0], abuf.at[a_slot(mat)], asem.at[a_slot(mat)]).wait()

        @pl.when((kind == 2) & (layer < layers - 1))
        def _():
            start_a(xt, layer + 1, 2 * lax.rem(layer + 1, 2))
            start_a(dt, layer + 1, 2 * lax.rem(layer + 1, 2) + 1)

    def read_part(mat):
        slot = lax.rem(mat, SLOTS)
        acc = jnp.zeros((p_loc, q_loc), jnp.float32)
        later = mat + SLOTS - 1
        for k in range(main):
            part = pl.ds(k * rows, rows)
            pltpu.make_async_copy(dyq.at[0, 0, part], bbuf.at[slot, part], bsem.at[slot, k]).wait()

            @pl.when(later < n_mats)
            def _():
                of_mat(start_piece, later, lax.rem(later, SLOTS), k)

            acc += product(mat, part, bbuf[slot, part, :])
        return acc

    def statistics(mat):
        block = g[mat]
        q_sq = block * block + EPS_SQUARE
        q_part = jnp.sum(q_sq, axis=0, keepdims=True)
        folded = q_sq[:, :LANES]
        for k in range(1, q_rows):
            folded += q_sq[:, k * LANES:(k + 1) * LANES]
        padded = jnp.concatenate([folded, jnp.zeros((LANES - p_loc, LANES), jnp.float32)], axis=0)
        for k in range(q_rows):
            qrecv[me_e, mat, k:k + 1, :] = q_part[:, k * LANES:(k + 1) * LANES]
        precv[me_a, mat] = jnp.sum(padded.T, axis=0, keepdims=True)

    def early(mat):
        ready_a(mat)
        acc = read_part(mat)
        wait_pass(mat)
        acc += product(mat, own_part, fbuf[mat])
        pltpu.make_async_copy(dyq.at[0, 0, pl.ds(0, rows)], rbuf.at[mat], rsem.at[mat]).wait()
        g[mat] = acc + product(mat, got_part, rbuf[mat])

    early(0)
    start_a(dt, 0, 1)
    start_pass(source(EARLY + 1), EARLY + 1)
    statistics(0)
    early(1)
    for mat in range(EARLY + 2, RING):
        start_pass(source(mat), mat)
    pl.semaphore_wait(barrier, n_dev - 1)
    for mat in range(EARLY, EARLY + LEAD):
        wait_pass(mat)
        pass_copy(mat).start()
    for mat in range(EARLY):
        pl.semaphore_signal(free_sem, inc=1, device_id=partner, device_id_type=MESH)
        start_pass(source(mat + RING), mat)
    for copy in small + w_copies:
        copy.start()

    def pass_ahead(mat):
        ahead = mat + LEAD

        @pl.when(ahead < n_mats)
        def _():
            @pl.when(ahead >= RING)
            def _():
                pl.semaphore_wait(free_sem, 1)

            wait_pass(lax.rem(ahead, RING))
            pass_copy(lax.rem(ahead, RING)).start()

    def add_passed(mat, acc):
        ring = lax.rem(mat, RING)
        pass_copy(ring).wait_recv()
        g[mat] = acc + product(mat, got_part, rbuf[ring])

        @pl.when(mat + RING < n_mats)
        def _():
            pl.semaphore_signal(free_sem, inc=1, device_id=partner, device_id_type=MESH)
            pass_copy(ring).wait_send()
            of_mat(start_pass, mat + RING, ring)

    def stream(mat, carry):
        pass_ahead(mat)
        ready_a(mat)
        acc = product(mat, own_part, fbuf[lax.rem(mat, RING)])
        statistics(mat - 1)
        add_passed(mat, acc + read_part(mat))
        return carry

    def wave_of(event):
        return max(event - layers + 2, 0)

    def q_copy(lo, hi, event, peer):
        span = qrecv.at[me_e, pl.ds(lo, hi - lo)]
        return pltpu.make_async_remote_copy(
            src_ref=span, dst_ref=span, send_sem=qsend_sem, recv_sem=qrecv_sem.at[wave_of(event)],
            device_id={"att": me_a, "emb": peer}, device_id_type=MESH)

    def p_copy(lo, hi, event, peer):
        span = precv.at[me_a, pl.ds(lo, hi - lo)]
        return pltpu.make_async_remote_copy(
            src_ref=span, dst_ref=span, send_sem=psend_sem, recv_sem=precv_sem.at[wave_of(event)],
            device_id={"att": peer, "emb": me_e}, device_id_type=MESH)

    def u_copy(target):
        return pltpu.make_async_remote_copy(
            src_ref=urecv.at[me], dst_ref=urecv.at[me], send_sem=usend_sem, recv_sem=urecv_sem,
            device_id=target, device_id_type=MESH)

    def send(lo, hi, event):
        for s in emb_steps:
            q_copy(lo, hi, event, emb_at[s]).start()
        for k in range(1, n_att):
            p_copy(lo, hi, event, att_at[k]).start()

    def wait_bytes(ref, sem):
        pltpu.make_async_copy(ref, ref, sem).wait()

    lane = lax.broadcasted_iota(jnp.int32, (1, LANES), 1)

    def process(lo, hi, wave, u_row):
        wait_bytes(qrecv.at[pl.ds(0, n_emb - 1), pl.ds(lo, hi - lo)], qrecv_sem.at[wave])
        wait_bytes(precv.at[pl.ds(0, n_att - 1), pl.ds(lo, hi - lo)], precv_sem.at[wave])
        beta = hv[0:1, 0:1]
        for mat in range(lo, hi):
            layer, kind = mat // MATS, mat % MATS
            is_out = kind == MATS - 1
            q_sum = qrecv[0, mat]
            for peer in range(1, n_emb):
                q_sum += qrecv[peer, mat]
            p_sum = precv[0, mat]
            for peer in range(1, n_att):
                p_sum += precv[peer, mat]
            q_add = (1.0 - beta) * (q_sum / d_model)
            p_new_all = (1.0 - beta) * (p_sum / inner)
            p_old = cov[layer:layer + 1, :] if is_out else rqv[kind, layer:layer + 1, :]
            p_new = beta * p_old + p_new_all[:, :p_loc]
            q_parts = []
            for k in range(q_rows):
                cols = slice(k * LANES, (k + 1) * LANES)
                q_old = rov[layer:layer + 1, cols] if is_out else cqv[kind, layer:layer + 1, cols]
                q_new = beta * q_old + q_add[k:k + 1, :]
                if is_out:
                    ro_new[layer:layer + 1, cols] = q_new
                else:
                    cq_new[kind, layer:layer + 1, cols] = q_new
                q_parts.append(q_new)
            if is_out:
                co_new[layer:layer + 1, :] = p_new
                r_total = jnp.sum(sum(q_parts[1:], q_parts[0]), axis=1, keepdims=True)
            else:
                rq_new[kind, layer:layer + 1, :] = p_new
                r_total = jnp.sum(p_new, axis=1, keepdims=True)
            p_fac = jnp.concatenate([lax.rsqrt(p_new), jnp.zeros((1, LANES - p_loc), jnp.float32)], axis=1)
            p_fac = jnp.broadcast_to(p_fac, (LANES, LANES)).T[:p_loc, :]
            u_sum = jnp.zeros((p_loc, LANES), jnp.float32)
            w_sum = jnp.zeros((p_loc, LANES), jnp.float32)
            for k in range(q_rows):
                cols = slice(k * LANES, (k + 1) * LANES)
                upd = (g[mat, :, cols] * p_fac) * lax.rsqrt(q_parts[k])
                g[mat, :, cols] = upd
                w = wov[layer, :, cols] if is_out else wqv[layer, kind, :, cols]
                u_sum += upd * upd
                w_sum += w * w
            u_total = jnp.sum(jnp.sum(u_sum, axis=0, keepdims=True), axis=1, keepdims=True)
            w_total = jnp.sum(jnp.sum(w_sum, axis=0, keepdims=True), axis=1, keepdims=True)
            copies = n_emb if is_out else n_att
            mean_row = r_total / (copies * (inner if is_out else d_model))
            u_row = jnp.where(lane == mat, u_total, u_row)
            u_row = jnp.where(lane == n_mats + mat, w_total, u_row)
            u_row = jnp.where(lane == 2 * n_mats + mat, mean_row, u_row)
        return u_row

    groups = [(MATS * layer, MATS * (layer + 1)) for layer in range(layers - 1)]
    groups += [(n_mats - MATS, n_mats - 2), (n_mats - 2, n_mats)]
    u_row = jnp.zeros((1, LANES), jnp.float32)
    done = EARLY
    for event, (lo, hi) in enumerate(groups):
        upto = min(hi + 1, n_mats)
        if hi < n_mats:
            lax.fori_loop(done, upto, stream, 0)
        else:
            stream(n_mats - 1, 0)
            statistics(n_mats - 1)
        done = upto
        send(lo, hi, event)
    for copy in small + w_copies:
        copy.wait()
    for wave, (lo, hi) in enumerate([(0, n_mats - MATS), *groups[-2:]]):
        u_row = process(lo, hi, wave, u_row)

    urecv[me] = u_row

    for k, s in all_steps:
        u_copy({"att": att_at[k], "emb": emb_at[s]}).start()
    wait_bytes(urecv.at[pl.ds(0, n_dev - 1)], urecv_sem)
    total = urecv[0]
    for peer in range(1, n_dev):
        total += urecv[peer]
    w_total = pltpu.roll(total, LANES - n_mats, 1)
    mean_row = pltpu.roll(total, LANES - 2 * n_mats, 1)
    n_elems = d_model * inner
    rel_step, clip_limit = hv[0:1, 1:2], hv[0:1, 2:3]
    rms_u = jnp.sqrt(mean_row * total / n_elems)
    rms_w = jnp.sqrt(w_total / n_elems)
    scale = rel_step * jnp.maximum(EPS_SCALE, rms_w) / jnp.maximum(1.0, rms_u / clip_limit) * jnp.sqrt(mean_row)
    scale_rows[...] = jnp.broadcast_to(scale, (LANES, LANES)).T[:n_mats, :]

    for mat in range(n_mats - RING, n_mats):
        pass_copy(mat % RING).wait_send()
    wait_bytes(qrecv.at[pl.ds(0, n_emb - 1)], qsend_sem)
    wait_bytes(precv.at[pl.ds(0, n_att - 1)], psend_sem)
    wait_bytes(urecv.at[pl.ds(0, n_dev - 1)], usend_sem)


def update_kernel(wqv, wov, g, scale_rows, *refs):
    stats, wq_new, wo_new, stats_new, wq_out, wo_out, sems = refs[:4], refs[4], refs[5], refs[6:10], *refs[10:]
    copies = [pltpu.make_async_copy(src, dst, sems.at[k]) for k, (src, dst) in enumerate(zip(stats, stats_new))]
    for copy in copies:
        copy.start()
    for mat in range(g.shape[0]):
        layer, kind = mat // MATS, mat % MATS
        step = jnp.concatenate([scale_rows[mat:mat + 1, :]] * (g.shape[2] // LANES), axis=1) * g[mat]
        if kind == MATS - 1:
            wo_out[layer] = wov[layer] - step
            copy = pltpu.make_async_copy(wo_out.at[layer], wo_new.at[layer], sems.at[len(stats) + mat])
        else:
            wq_out[layer, kind] = wqv[layer, kind] - step
            copy = pltpu.make_async_copy(wq_out.at[layer, kind], wq_new.at[layer, kind], sems.at[len(stats) + mat])
        copy.start()
        copies.append(copy)
    for copy in copies:
        copy.wait()


def solution(mesh):
    n_emb = mesh.shape["emb"]
    n_att = mesh.shape["att"]
    in_specs = (
        P(None, None, "emb", "att"),
        P(None, "att", "emb"),
        P(None, None, "emb"),
        P(None, None, None, "att"),
        P(None, None, "att"),
        P(None, None, "emb"),
        P(None, None, "emb"),
        P(None, None, "att"),
        P(None, "att"),
        P(None, "emb"),
        P(),
    )
    out_specs = (
        P(None, None, "emb", "att"),
        P(None, "att", "emb"),
        P(None, None, "emb"),
        P(None, None, "att"),
        P(None, "att"),
        P(None, "emb"),
    )

    def local_run(w_qkv, w_out, x_in, dy_qkv, x_attn, dy_out, r_qkv, c_qkv, r_out, c_out, hyper_params):
        f32, bf16 = jnp.float32, jnp.bfloat16
        layers, tokens, p_loc = x_in.shape
        q_loc = x_attn.shape[2]
        n_mats = layers * MATS
        rows = tokens // PIECES
        args = (
            jnp.swapaxes(x_in, 1, 2), jnp.swapaxes(dy_out, 1, 2), dy_qkv, x_attn,
            w_qkv, jnp.swapaxes(w_out, 1, 2),
            jnp.swapaxes(r_qkv, 0, 1), jnp.swapaxes(c_qkv, 0, 1), r_out, c_out, hyper_params.reshape(1, 3),
        )
        args = tuple(pltpu.with_memory_space_constraint(a, pltpu.HBM) for a in args)
        sds = jax.ShapeDtypeStruct
        wo_shape = (layers, p_loc, q_loc)
        rq_shape, cq_shape = (3, layers, p_loc), (3, layers, q_loc)
        w_shape = (sds(w_qkv.shape, f32), sds(wo_shape, f32))
        stat_shape = (sds(rq_shape, f32), sds(cq_shape, f32), sds(r_out.shape, f32), sds(c_out.shape, f32))
        held = (*w_shape, sds((n_mats, p_loc, q_loc), f32), sds((n_mats, LANES), f32), *stat_shape)
        dma = pltpu.SemaphoreType.DMA
        outs = pl.pallas_call(
            functools.partial(adafactor_kernel, n_att, n_emb),
            out_shape=held,
            in_specs=[pl.BlockSpec(memory_space=pltpu.HBM)] * len(args),
            out_specs=[pl.BlockSpec(memory_space=pltpu.VMEM)] * len(held),
            scratch_shapes=[
                pltpu.VMEM((SLOTS, tokens - 2 * rows, q_loc), bf16),
                pltpu.VMEM((RING, rows, q_loc), bf16),
                pltpu.VMEM((RING, rows, q_loc), bf16),
                pltpu.VMEM((4, p_loc, tokens), bf16),
                pltpu.VMEM(rq_shape, f32),
                pltpu.VMEM(cq_shape, f32),
                pltpu.VMEM(r_out.shape, f32),
                pltpu.VMEM(c_out.shape, f32),
                pltpu.VMEM((1, 3), f32),
                pltpu.VMEM((n_emb, n_mats, q_loc // LANES, LANES), f32),
                pltpu.VMEM((n_att, n_mats, 1, LANES), f32),
                pltpu.VMEM((n_att * n_emb, 1, LANES), f32),
                dma((SLOTS, PIECES - 2)), dma((RING,)), dma((RING,)), dma((RING,)), pltpu.SemaphoreType.REGULAR,
                dma((4,)), dma((2,)), dma((5,)),
                dma(()), dma((3,)), dma(()), dma((3,)), dma(()), dma(()),
            ],
            compiler_params=pltpu.CompilerParams(
                collective_id=0, has_side_effects=True, vmem_limit_bytes=42 * 1024 * 1024),
            name="adafactor",
        )(*args)
        outs = pl.pallas_call(
            update_kernel,
            out_shape=(*w_shape, *stat_shape),
            in_specs=[pl.BlockSpec(memory_space=pltpu.VMEM)] * len(held),
            out_specs=[pl.BlockSpec(memory_space=pltpu.HBM)] * (len(w_shape) + len(stat_shape)),
            scratch_shapes=[
                pltpu.VMEM(w_qkv.shape, f32), pltpu.VMEM(wo_shape, f32), dma((len(stat_shape) + n_mats,)),
            ],
            compiler_params=pltpu.CompilerParams(vmem_limit_bytes=4 * 1024 * 1024),
            name="update",
        )(*outs)
        return (
            outs[0], jnp.swapaxes(outs[1], 1, 2), jnp.swapaxes(outs[2], 0, 1), jnp.swapaxes(outs[3], 0, 1),
            outs[4], outs[5],
        )

    return jax.shard_map(local_run, mesh=mesh, in_specs=in_specs, out_specs=out_specs, check_vma=False)
```

```python
import functools
import jax
import jax.numpy as jnp
from jax import lax
from jax.experimental import pallas as pl
from jax.experimental.pallas import tpu as pltpu
from jax.sharding import PartitionSpec as P

EPS_SQUARE = 1e-30
EPS_SCALE = 1e-3
LANES = 128
MATS = 4
SLOTS = 3
PIECES = 6
RING = 5
LEAD = 1
EARLY = 2
MESH = pl.DeviceIdType.MESH


def tree_sum(terms):
    while len(terms) > 1:
        terms = [a + b for a, b in zip(terms[::2], terms[1::2])] + terms[len(terms) // 2 * 2:]
    return terms[0]


def adafactor_kernel(
    n_att, n_emb,
    xt, dt, dyq, xa, wq, wo, rq, cq, ro, co, hyp,
    wqv, wov, g, scale_rows, rq_new, cq_new, ro_new, co_new,
    bbuf, fbuf, rbuf, abuf, rqv, cqv, rov, cov, hv, qrecv, precv, urecv,
    bsem, fsem, fsend_sem, rsem, free_sem, asem, wsem, ssem,
    qsend_sem, qrecv_sem, psend_sem, precv_sem, usend_sem, urecv_sem,
):
    layers, p_loc, tokens = xt.shape
    q_loc = dyq.shape[3]
    n_mats = layers * MATS
    n_dev = n_att * n_emb
    d_model, inner = p_loc * n_emb, q_loc * n_att
    rows, main = tokens // PIECES, PIECES - 2
    q_rows = q_loc // LANES
    me_a, me_e = lax.axis_index("att"), lax.axis_index("emb")
    me = me_a * n_emb + me_e
    core = lax.rem(me_e, 2)
    partner = {"att": me_a, "emb": me_e + 1 - 2 * core}
    own_part = pl.ds(pl.multiple_of((PIECES - 1 - core) * rows, rows), rows)
    got_part = pl.ds(pl.multiple_of((PIECES - 2 + core) * rows, rows), rows)

    def start_a(src, layer, slot):
        pltpu.make_async_copy(src.at[layer], abuf.at[slot], asem.at[slot]).start()

    def start_pass(src, slot):
        pltpu.make_async_copy(src.at[own_part], fbuf.at[slot], fsem.at[slot]).start()

    def start_got(src, slot):
        pltpu.make_async_copy(src.at[got_part], rbuf.at[slot], rsem.at[slot]).start()

    def start_piece(src, slot, k):
        part = pl.ds(k * rows, rows)
        pltpu.make_async_copy(src.at[part], bbuf.at[slot, part], bsem.at[slot, k]).start()

    def of_mat(start, mat, slot, *more):
        layer, kind = mat // MATS, lax.rem(mat, MATS)

        @pl.when(kind < MATS - 1)
        def _():
            start(dyq.at[layer, kind], slot, *more)

        @pl.when(kind == MATS - 1)
        def _():
            start(xa.at[layer], slot, *more)

    def source(mat):
        return xa.at[mat // MATS] if mat % MATS == MATS - 1 else dyq.at[mat // MATS, mat % MATS]

    start_a(xt, 0, 0)
    for k in range(main):
        start_piece(source(0), 0, k)
    start_pass(source(0), 0)
    start_got(source(0), 0)
    small = [
        pltpu.make_async_copy(src, dst, ssem.at[k])
        for k, (src, dst) in enumerate([(rq, rqv), (cq, cqv), (ro, rov), (co, cov), (hyp, hv)])
    ]
    w_copies = [pltpu.make_async_copy(wq, wqv, wsem.at[0]), pltpu.make_async_copy(wo, wov, wsem.at[1])]

    side = 4
    att_at = [lax.rem(me_a + k, n_att) for k in range(n_att)]
    planes = n_emb // (2 * side)
    z_at = [lax.rem(me_e // (2 * side) + k, planes) * (2 * side) for k in range(planes)]
    y_at = [lax.rem(lax.rem(me_e, 2 * side) // 2 + k, side) * 2 for k in range(side)]
    core_at = [core, 1 - core]

    def hops(k, n):
        return min(k, n - k)

    emb_steps = sorted(
        ((z, y, h) for z in range(planes) for y in range(side) for h in range(2) if (z, y, h) != (0, 0, 0)),
        key=lambda s: -(hops(s[0], planes) + hops(s[1], side)))
    emb_at = {(z, y, h): z_at[z] + y_at[y] + core_at[h] for z in range(planes) for y in range(side) for h in range(2)}
    all_steps = sorted(
        ((k, s) for k in range(n_att) for s in emb_at if (k, s) != (0, (0, 0, 0))),
        key=lambda t: -(hops(t[0], n_att) + hops(t[1][0], planes) + hops(t[1][1], side)))

    barrier = pltpu.get_barrier_semaphore()
    for k, s in all_steps:
        pl.semaphore_signal(
            barrier, inc=1, device_id={"att": att_at[k], "emb": emb_at[s]}, device_id_type=MESH)
    for k in range(main):
        start_piece(source(1), 1, k)
    start_pass(source(1), 1)
    start_got(source(1), 1)
    start_pass(source(EARLY), EARLY)

    def pass_copy(slot):
        return pltpu.make_async_remote_copy(
            src_ref=fbuf.at[slot], dst_ref=rbuf.at[slot], send_sem=fsend_sem.at[slot], recv_sem=rsem.at[slot],
            device_id=partner, device_id_type=MESH)

    def wait_pass(slot):
        pltpu.make_async_copy(dyq.at[0, 0, pl.ds(0, rows)], fbuf.at[slot], fsem.at[slot]).wait()

    def a_slot(mat):
        return 2 * lax.rem(mat // MATS, 2) + lax.rem(mat, MATS) // (MATS - 1)

    def product(mat, part, b):
        return jnp.dot(abuf[a_slot(mat), :, part], b, preferred_element_type=jnp.float32)

    def ready_a(mat):
        kind, layer = lax.rem(mat, MATS), mat // MATS

        @pl.when(lax.rem(kind, MATS - 1) == 0)
        def _():
            pltpu.make_async_copy(xt.at[0], abuf.at[a_slot(mat)], asem.at[a_slot(mat)]).wait()

        @pl.when((kind == 2) & (layer < layers - 1))
        def _():
            start_a(xt, layer + 1, 2 * lax.rem(layer + 1, 2))
            start_a(dt, layer + 1, 2 * lax.rem(layer + 1, 2) + 1)

    def read_part(mat):
        slot = lax.rem(mat, SLOTS)
        acc = jnp.zeros((p_loc, q_loc), jnp.float32)
        later = mat + SLOTS - 1
        for k in range(main):
            part = pl.ds(k * rows, rows)
            pltpu.make_async_copy(dyq.at[0, 0, part], bbuf.at[slot, part], bsem.at[slot, k]).wait()

            @pl.when(later < n_mats)
            def _():
                of_mat(start_piece, later, lax.rem(later, SLOTS), k)

            acc += product(mat, part, bbuf[slot, part, :])
        return acc

    def statistics(mat):
        block = g[mat]
        q_sq = block * block + EPS_SQUARE
        q_part = jnp.sum(q_sq, axis=0, keepdims=True)
        folded = q_sq[:, :LANES]
        for k in range(1, q_rows):
            folded += q_sq[:, k * LANES:(k + 1) * LANES]
        padded = jnp.concatenate([folded, jnp.zeros((LANES - p_loc, LANES), jnp.float32)], axis=0)
        for k in range(q_rows):
            qrecv[me_e, mat, k:k + 1, :] = q_part[:, k * LANES:(k + 1) * LANES]
        precv[me_a, mat] = jnp.sum(padded.T, axis=0, keepdims=True)

    def early(mat):
        ready_a(mat)
        acc = read_part(mat)
        wait_pass(mat)
        acc += product(mat, own_part, fbuf[mat])
        pltpu.make_async_copy(dyq.at[0, 0, pl.ds(0, rows)], rbuf.at[mat], rsem.at[mat]).wait()
        g[mat] = acc + product(mat, got_part, rbuf[mat])

    early(0)
    start_a(dt, 0, 1)
    start_pass(source(EARLY + 1), EARLY + 1)
    statistics(0)
    early(1)
    for mat in range(EARLY + 2, RING):
        start_pass(source(mat), mat)
    pl.semaphore_wait(barrier, n_dev - 1)
    for mat in range(EARLY, EARLY + LEAD):
        wait_pass(mat)
        pass_copy(mat).start()
    for mat in range(EARLY):
        pl.semaphore_signal(free_sem, inc=1, device_id=partner, device_id_type=MESH)
        start_pass(source(mat + RING), mat)
    for copy in small:
        copy.start()

    def pass_ahead(mat):
        ahead = mat + LEAD

        @pl.when(ahead < n_mats)
        def _():
            @pl.when(ahead >= RING)
            def _():
                pl.semaphore_wait(free_sem, 1)

            wait_pass(lax.rem(ahead, RING))
            pass_copy(lax.rem(ahead, RING)).start()

    def add_passed(mat, acc):
        ring = lax.rem(mat, RING)
        pass_copy(ring).wait_recv()
        g[mat] = acc + product(mat, got_part, rbuf[ring])

        @pl.when(mat + RING < n_mats)
        def _():
            pl.semaphore_signal(free_sem, inc=1, device_id=partner, device_id_type=MESH)
            pass_copy(ring).wait_send()
            of_mat(start_pass, mat + RING, ring)

    def stream(mat, carry):
        pass_ahead(mat)
        ready_a(mat)
        acc = product(mat, own_part, fbuf[lax.rem(mat, RING)])
        statistics(mat - 1)
        add_passed(mat, acc + read_part(mat))
        return carry

    def wave_of(event):
        return max(event - layers + 2, 0)

    def q_copy(lo, hi, event, peer):
        span = qrecv.at[me_e, pl.ds(lo, hi - lo)]
        return pltpu.make_async_remote_copy(
            src_ref=span, dst_ref=span, send_sem=qsend_sem, recv_sem=qrecv_sem.at[wave_of(event)],
            device_id={"att": me_a, "emb": peer}, device_id_type=MESH)

    def p_copy(lo, hi, event, peer):
        span = precv.at[me_a, pl.ds(lo, hi - lo)]
        return pltpu.make_async_remote_copy(
            src_ref=span, dst_ref=span, send_sem=psend_sem, recv_sem=precv_sem.at[wave_of(event)],
            device_id={"att": peer, "emb": me_e}, device_id_type=MESH)

    def u_copy(target):
        return pltpu.make_async_remote_copy(
            src_ref=urecv.at[me], dst_ref=urecv.at[me], send_sem=usend_sem, recv_sem=urecv_sem,
            device_id=target, device_id_type=MESH)

    def send(lo, hi, event):
        for s in emb_steps:
            q_copy(lo, hi, event, emb_at[s]).start()
        for k in range(1, n_att):
            p_copy(lo, hi, event, att_at[k]).start()

    def wait_bytes(ref, sem):
        pltpu.make_async_copy(ref, ref, sem).wait()

    lane = lax.broadcasted_iota(jnp.int32, (1, LANES), 1)

    def process(lo, hi, wave, u_row):
        wait_bytes(qrecv.at[pl.ds(0, n_emb - 1), pl.ds(lo, hi - lo)], qrecv_sem.at[wave])
        wait_bytes(precv.at[pl.ds(0, n_att - 1), pl.ds(lo, hi - lo)], precv_sem.at[wave])
        beta = hv[0:1, 0:1]
        for mat in range(lo, hi):
            layer, kind = mat // MATS, mat % MATS
            is_out = kind == MATS - 1
            q_sum = tree_sum([qrecv[peer, mat] for peer in range(n_emb)])
            p_sum = tree_sum([precv[peer, mat] for peer in range(n_att)])
            q_add = (1.0 - beta) * (q_sum / d_model)
            p_new_all = (1.0 - beta) * (p_sum / inner)
            p_old = cov[layer:layer + 1, :] if is_out else rqv[kind, layer:layer + 1, :]
            p_new = beta * p_old + p_new_all[:, :p_loc]
            q_parts = []
            for k in range(q_rows):
                cols = slice(k * LANES, (k + 1) * LANES)
                q_old = rov[layer:layer + 1, cols] if is_out else cqv[kind, layer:layer + 1, cols]
                q_new = beta * q_old + q_add[k:k + 1, :]
                if is_out:
                    ro_new[layer:layer + 1, cols] = q_new
                else:
                    cq_new[kind, layer:layer + 1, cols] = q_new
                q_parts.append(q_new)
            if is_out:
                co_new[layer:layer + 1, :] = p_new
                r_total = jnp.sum(sum(q_parts[1:], q_parts[0]), axis=1, keepdims=True)
            else:
                rq_new[kind, layer:layer + 1, :] = p_new
                r_total = jnp.sum(p_new, axis=1, keepdims=True)
            p_fac = jnp.concatenate([lax.rsqrt(p_new), jnp.zeros((1, LANES - p_loc), jnp.float32)], axis=1)
            p_fac = jnp.broadcast_to(p_fac, (LANES, LANES)).T[:p_loc, :]
            u_sum = jnp.zeros((p_loc, LANES), jnp.float32)
            w_sum = jnp.zeros((p_loc, LANES), jnp.float32)
            for k in range(q_rows):
                cols = slice(k * LANES, (k + 1) * LANES)
                upd = (g[mat, :, cols] * p_fac) * lax.rsqrt(q_parts[k])
                g[mat, :, cols] = upd
                w = wov[layer, :, cols] if is_out else wqv[layer, kind, :, cols]
                u_sum += upd * upd
                w_sum += w * w
            u_total = jnp.sum(jnp.sum(u_sum, axis=0, keepdims=True), axis=1, keepdims=True)
            w_total = jnp.sum(jnp.sum(w_sum, axis=0, keepdims=True), axis=1, keepdims=True)
            copies = n_emb if is_out else n_att
            mean_row = r_total / (copies * (inner if is_out else d_model))
            u_row = jnp.where(lane == mat, u_total, u_row)
            u_row = jnp.where(lane == n_mats + mat, w_total, u_row)
            u_row = jnp.where(lane == 2 * n_mats + mat, mean_row, u_row)
        return u_row

    groups = [(MATS * layer, MATS * (layer + 1)) for layer in range(layers - 1)]
    groups += [(n_mats - MATS, n_mats - 2), (n_mats - 2, n_mats)]
    u_row = jnp.zeros((1, LANES), jnp.float32)
    done = EARLY
    for event, (lo, hi) in enumerate(groups):
        upto = min(hi + 1, n_mats)
        if hi < n_mats:
            lax.fori_loop(done, upto, stream, 0)
        else:
            stream(n_mats - 1, 0)
            for copy in w_copies:
                copy.start()
            statistics(n_mats - 1)
        done = upto
        send(lo, hi, event)
    for copy in small + w_copies:
        copy.wait()
    for wave, (lo, hi) in enumerate([(0, n_mats - MATS), *groups[-2:]]):
        u_row = process(lo, hi, wave, u_row)

    urecv[me] = u_row

    for k, s in all_steps:
        u_copy({"att": att_at[k], "emb": emb_at[s]}).start()
    wait_bytes(urecv.at[pl.ds(0, n_dev - 1)], urecv_sem)
    total = tree_sum([urecv[peer] for peer in range(n_dev)])
    w_total = pltpu.roll(total, LANES - n_mats, 1)
    mean_row = pltpu.roll(total, LANES - 2 * n_mats, 1)
    n_elems = d_model * inner
    rel_step, clip_limit = hv[0:1, 1:2], hv[0:1, 2:3]
    rms_u = jnp.sqrt(mean_row * total / n_elems)
    rms_w = jnp.sqrt(w_total / n_elems)
    scale = rel_step * jnp.maximum(EPS_SCALE, rms_w) / jnp.maximum(1.0, rms_u / clip_limit) * jnp.sqrt(mean_row)
    scale_rows[...] = jnp.broadcast_to(scale, (LANES, LANES)).T[:n_mats, :]

    for mat in range(n_mats - RING, n_mats):
        pass_copy(mat % RING).wait_send()
    wait_bytes(qrecv.at[pl.ds(0, n_emb - 1)], qsend_sem)
    wait_bytes(precv.at[pl.ds(0, n_att - 1)], psend_sem)
    wait_bytes(urecv.at[pl.ds(0, n_dev - 1)], usend_sem)


def update_kernel(wqv, wov, g, scale_rows, *refs):
    stats, wq_new, wo_new, stats_new, wq_out, wo_out, sems = refs[:4], refs[4], refs[5], refs[6:10], *refs[10:]
    copies = [pltpu.make_async_copy(src, dst, sems.at[k]) for k, (src, dst) in enumerate(zip(stats, stats_new))]
    for copy in copies:
        copy.start()
    for mat in range(g.shape[0]):
        layer, kind = mat // MATS, mat % MATS
        step = jnp.concatenate([scale_rows[mat:mat + 1, :]] * (g.shape[2] // LANES), axis=1) * g[mat]
        if kind == MATS - 1:
            wo_out[layer] = wov[layer] - step
            copy = pltpu.make_async_copy(wo_out.at[layer], wo_new.at[layer], sems.at[len(stats) + mat])
        else:
            wq_out[layer, kind] = wqv[layer, kind] - step
            copy = pltpu.make_async_copy(wq_out.at[layer, kind], wq_new.at[layer, kind], sems.at[len(stats) + mat])
        copy.start()
        copies.append(copy)
    for copy in copies:
        copy.wait()


def solution(mesh):
    n_emb = mesh.shape["emb"]
    n_att = mesh.shape["att"]
    in_specs = (
        P(None, None, "emb", "att"),
        P(None, "att", "emb"),
        P(None, None, "emb"),
        P(None, None, None, "att"),
        P(None, None, "att"),
        P(None, None, "emb"),
        P(None, None, "emb"),
        P(None, None, "att"),
        P(None, "att"),
        P(None, "emb"),
        P(),
    )
    out_specs = (
        P(None, None, "emb", "att"),
        P(None, "att", "emb"),
        P(None, None, "emb"),
        P(None, None, "att"),
        P(None, "att"),
        P(None, "emb"),
    )

    def local_run(w_qkv, w_out, x_in, dy_qkv, x_attn, dy_out, r_qkv, c_qkv, r_out, c_out, hyper_params):
        f32, bf16 = jnp.float32, jnp.bfloat16
        layers, tokens, p_loc = x_in.shape
        q_loc = x_attn.shape[2]
        n_mats = layers * MATS
        rows = tokens // PIECES
        args = (
            jnp.swapaxes(x_in, 1, 2), jnp.swapaxes(dy_out, 1, 2), dy_qkv, x_attn,
            w_qkv, jnp.swapaxes(w_out, 1, 2),
            jnp.swapaxes(r_qkv, 0, 1), jnp.swapaxes(c_qkv, 0, 1), r_out, c_out, hyper_params.reshape(1, 3),
        )
        args = tuple(pltpu.with_memory_space_constraint(a, pltpu.HBM) for a in args)
        sds = jax.ShapeDtypeStruct
        wo_shape = (layers, p_loc, q_loc)
        rq_shape, cq_shape = (3, layers, p_loc), (3, layers, q_loc)
        w_shape = (sds(w_qkv.shape, f32), sds(wo_shape, f32))
        stat_shape = (sds(rq_shape, f32), sds(cq_shape, f32), sds(r_out.shape, f32), sds(c_out.shape, f32))
        held = (*w_shape, sds((n_mats, p_loc, q_loc), f32), sds((n_mats, LANES), f32), *stat_shape)
        dma = pltpu.SemaphoreType.DMA
        outs = pl.pallas_call(
            functools.partial(adafactor_kernel, n_att, n_emb),
            out_shape=held,
            in_specs=[pl.BlockSpec(memory_space=pltpu.HBM)] * len(args),
            out_specs=[pl.BlockSpec(memory_space=pltpu.VMEM)] * len(held),
            scratch_shapes=[
                pltpu.VMEM((SLOTS, tokens - 2 * rows, q_loc), bf16),
                pltpu.VMEM((RING, rows, q_loc), bf16),
                pltpu.VMEM((RING, rows, q_loc), bf16),
                pltpu.VMEM((4, p_loc, tokens), bf16),
                pltpu.VMEM(rq_shape, f32),
                pltpu.VMEM(cq_shape, f32),
                pltpu.VMEM(r_out.shape, f32),
                pltpu.VMEM(c_out.shape, f32),
                pltpu.VMEM((1, 3), f32),
                pltpu.VMEM((n_emb, n_mats, q_loc // LANES, LANES), f32),
                pltpu.VMEM((n_att, n_mats, 1, LANES), f32),
                pltpu.VMEM((n_att * n_emb, 1, LANES), f32),
                dma((SLOTS, PIECES - 2)), dma((RING,)), dma((RING,)), dma((RING,)), pltpu.SemaphoreType.REGULAR,
                dma((4,)), dma((2,)), dma((5,)),
                dma(()), dma((3,)), dma(()), dma((3,)), dma(()), dma(()),
            ],
            compiler_params=pltpu.CompilerParams(
                collective_id=0, has_side_effects=True, vmem_limit_bytes=42 * 1024 * 1024),
            name="adafactor",
        )(*args)
        outs = pl.pallas_call(
            update_kernel,
            out_shape=(*w_shape, *stat_shape),
            in_specs=[pl.BlockSpec(memory_space=pltpu.VMEM)] * len(held),
            out_specs=[pl.BlockSpec(memory_space=pltpu.HBM)] * (len(w_shape) + len(stat_shape)),
            scratch_shapes=[
                pltpu.VMEM(w_qkv.shape, f32), pltpu.VMEM(wo_shape, f32), dma((len(stat_shape) + n_mats,)),
            ],
            compiler_params=pltpu.CompilerParams(vmem_limit_bytes=4 * 1024 * 1024),
            name="update",
        )(*outs)
        return (
            outs[0], jnp.swapaxes(outs[1], 1, 2), jnp.swapaxes(outs[2], 0, 1), jnp.swapaxes(outs[3], 0, 1),
            outs[4], outs[5],
        )

    return jax.shard_map(local_run, mesh=mesh, in_specs=in_specs, out_specs=out_specs, check_vma=False)
```
